256 devices in a mesh: rows: 32 (over z, y), cols: 8 (over x, core).
Axes of the slice: x: 4, y: 4, z: 8, core: 2. Of those that a mesh axis runs over, the one named last changes fastest.
Arguments:
- weight_up: bfloat16 [12288, 49152], P('rows', 'cols'), may hold values from -0.109375 to 0.109375
- low_up: bfloat16 [12288, 64], P('rows'), may hold values from -0.0546875 to 0.0546875
- high_up: bfloat16 [64, 49152], P(None, 'cols'), may hold values from -0.75 to 0.75
- norm_train: float32 [12288], P(('rows', 'cols')), may hold values from 0.25 to 1.75
- norm_step: float32 [12288], P(('rows', 'cols')), may hold values from -0.3 to 0.3
Outputs:
- serve_up: bfloat16 [12288, 49152], P(None, ('cols', 'rows'))
- scale_up: float32 [49152], P(('cols', 'rows'))
- serve_norm: bfloat16 [12288], replicated
The draws below stay inside these ranges and needn't reach their ends.
All inputs are finite; a program needn't handle non-finite values.
Results may differ from the reference program's by a relative error of at most 0.0004.
Values may be sent and summed in bfloat16 or wider, within the bound.
A program may use at most 64 MiB of HBM per device.

```python
import jax
import jax.numpy as jnp
from jax import lax

D_MODEL = 12288
D_INNER = 49152
RANK = 64


def raised(array, own_key, source, target, parts, factor):
    owner, partner = [(jnp.arange(array.shape[position]) // (array.shape[position] // parts)).reshape([-1 if axis == position else 1 for axis in range(array.ndim)]) for position in (source, target)]
    chosen = jax.random.permutation(own_key, parts)[partner]
    strong = (owner == chosen) | (owner == (partner + parts // 2) % parts)
    return jnp.where(strong, factor * array, array)


def shard_levels(own_key, shape, cuts, smallest, largest):
    level = 1.0
    for position, shards_of in cuts:
        draws = jax.random.uniform(jax.random.fold_in(jax.random.fold_in(own_key, 6), position), (shards_of,), jnp.float32, smallest / len(cuts), largest / len(cuts))
        level = level * jnp.repeat(jnp.exp(draws), shape[position] // shards_of).reshape((-1,) + (1,) * (len(shape) - 1 - position))
    return level


def gaussian(own_key, dims, width, limit, cuts=(), held_as=jnp.bfloat16):
    array = jax.random.normal(own_key, dims, jnp.float32) * width
    if len(cuts) > 0:
        array = shard_levels(own_key, dims, cuts, -0.22, 0.18) * array
    return jnp.clip(array, min=-limit, max=limit).astype(held_as)


def heavy_noise(key, dims, deviation, reach, shards, heavy, held_as=jnp.bfloat16):
    entries = deviation * jax.random.normal(key, dims, jnp.float32)
    if shards:
        entries = entries * shard_levels(key, dims, shards, -0.22, 0.18)
    return jnp.clip(raised(entries, jax.random.fold_in(key, 3), *heavy), -reach, reach).astype(held_as)


def setup_inputs(seed: int = 0) -> dict:
    key_of = jax.random.split(jax.random.key(seed), 6)
    return {
        "weight_up": heavy_noise(key_of[0], (D_MODEL, D_INNER), D_MODEL ** -0.5, 0.109375, ((0, 32), (1, 8)), (0, 1, 32, 2.75)),
        "low_up": gaussian(key_of[1], (D_MODEL, RANK), D_MODEL ** -0.5, 0.0546875, ((0, 32),)),
        "high_up": gaussian(key_of[2], (RANK, D_INNER), RANK ** -0.5, 0.75, ((1, 8),)),
        "norm_train": jnp.clip(1.0 + 0.15 * jax.random.normal(key_of[3], (D_MODEL,), jnp.float32), 0.25, 1.75),
        "norm_step": jnp.clip(jax.random.uniform(key_of[4], (D_MODEL,), jnp.float32, -0.3, 0.3) * shard_levels(key_of[4], (D_MODEL,), ((0, 256),), -0.4, 0.0), -0.3, 0.3),
    }


mix_rate = 0.5

def reference(weight_up, low_up, high_up, norm_train, norm_step):
    fresh_up = weight_up.astype(jnp.float32) + mix_rate * jnp.dot(low_up, high_up, preferred_element_type=jnp.float32)
    scale_up = jnp.sqrt(lax.optimization_barrier(jnp.sum(fresh_up * fresh_up, axis=0)))
    serve_up = (fresh_up / scale_up).astype(jnp.bfloat16)
    serve_norm = (norm_train + norm_step).astype(jnp.bfloat16)
    return (serve_up, scale_up, serve_norm)
```

```python
import functools

import jax
import jax.numpy as jnp
from jax import lax
from jax.experimental import pallas as pl
from jax.experimental.pallas import tpu as pltpu
from jax.sharding import Mesh
from jax.sharding import PartitionSpec as P

MESH = pl.DeviceIdType.MESH
Z, Y, X, C = 8, 4, 4, 2
PLANE = Z * Y
D_MODEL, RANK = 12288, 64
ROWS = D_MODEL // PLANE
COLS = 6144
MINE = COLS // PLANE
PIECE = D_MODEL // (PLANE * X * C)
STRIDE = 13

mix_rate = 0.5


def comm_kernel(
    w_hbm, low_hbm, high_hbm, train_hbm, step_hbm,
    fresh_ref, inv_ref, scale_ref, norm_ref,
    wbuf, stage, recv, lowbuf, nbuf, hpair, ht, acc, low_ref, nt_ref, ns_ref,
    wsem, isem, ssend, srecv, nsend, nrecv, psend, precv,
):
    z, y = lax.axis_index("z"), lax.axis_index("y")
    x, c = lax.axis_index("x"), lax.axis_index("c")
    row = z * Y + y

    def plane_device(dz, dy):
        return {"z": lax.rem(z + dz, Z), "y": lax.rem(y + dy, Y)}

    def side_device(k):
        other = lax.rem(x * C + c + k, X * C)
        return {"x": other // C, "c": lax.rem(other, C)}

    def weight_copy(p):
        return pltpu.make_async_copy(
            w_hbm.at[:, pl.ds(pl.multiple_of(p * 2 * MINE, 128), 2 * MINE)], wbuf.at[p], wsem.at[p]
        )

    for p in range(PLANE // 2):
        weight_copy(p).start()
    pair = high_hbm.at[:, pl.ds(pl.multiple_of((row // 2) * 2 * MINE, 128), 2 * MINE)]
    small = [
        pltpu.make_async_copy(ref, to, isem.at[k])
        for k, (ref, to) in enumerate(((train_hbm, nt_ref), (step_hbm, ns_ref), (low_hbm, low_ref), (pair, hpair)))
    ]
    for copy in small:
        copy.start()

    barrier = pltpu.get_barrier_semaphore()
    for d in range(1, PLANE):
        pl.semaphore_signal(barrier, inc=1, device_id=plane_device(d // Y, d % Y), device_id_type=MESH)
    for k in range(1, X * C):
        pl.semaphore_signal(barrier, inc=1, device_id=side_device(k), device_id_type=MESH)

    me = x * C + c
    for copy in small:
        copy.wait()
    gain = (nt_ref[...] + ns_ref[...]).astype(jnp.bfloat16).astype(jnp.float32)
    spot = me * PIECE + lax.broadcasted_iota(jnp.int32, (16, PIECE), 1)
    in_row = spot // 128 == lax.broadcasted_iota(jnp.int32, (16, PIECE), 0)
    left = jnp.where(in_row, jnp.broadcast_to(gain, (16, PIECE)), 0.0).astype(jnp.bfloat16)
    lane = lax.rem(me * PIECE + lax.broadcasted_iota(jnp.int32, (PIECE, 128), 0), 128)
    right = jnp.where(lane == lax.broadcasted_iota(jnp.int32, (PIECE, 128), 1), 1.0, 0.0).astype(jnp.bfloat16)
    nbuf[me] = jnp.dot(left, right, preferred_element_type=jnp.float32).astype(jnp.bfloat16)

    lowbuf[x, z, y, :, 0:ROWS] = low_ref[pl.ds(pl.multiple_of(x * 16, 16), 16), :]

    wide = jnp.concatenate([hpair[...].astype(jnp.float32), jnp.zeros((RANK, 2 * MINE), jnp.float32)], axis=0)
    ht[...] = wide.T
    mine = pl.ds(pl.multiple_of(lax.rem(row, 2) * MINE, 8), MINE)
    high_t = ht[mine, :][:, 0:RANK].astype(jnp.bfloat16)

    @pl.loop(0, PLANE // 2)
    def _(p):
        weight_copy(p).wait()
        turned = wbuf[p].T
        stage[2 * p] = turned[0:MINE]
        stage[2 * p + 1] = turned[MINE : 2 * MINE]

    pl.semaphore_wait(barrier, PLANE - 1 + X * C - 1)

    def block_copy(d):
        dz, dy = d // Y, lax.rem(d, Y)
        to_z, to_y = lax.rem(z + dz, Z), lax.rem(y + dy, Y)
        return pltpu.make_async_remote_copy(
            src_ref=stage.at[to_z * Y + to_y], dst_ref=recv.at[d], send_sem=ssend.at[d], recv_sem=srecv.at[d],
            device_id={"z": to_z, "y": to_y}, device_id_type=MESH,
        )

    def send_blocks(first, last):
        @pl.loop(first, last)
        def _(i):
            block_copy(lax.rem(i * STRIDE, PLANE)).start()

    send_blocks(1, 5)

    def gain_copy(k):
        return pltpu.make_async_remote_copy(
            src_ref=nbuf.at[me], dst_ref=nbuf.at[me], send_sem=nsend.at[k], recv_sem=nrecv.at[k],
            device_id=side_device(k), device_id_type=MESH,
        )

    for k in range(1, X * C):
        gain_copy(k).start()
    for k in range(1, X * C):
        gain_copy(k).wait()
    gains = nbuf[0].astype(jnp.float32)
    for k in range(1, X * C):
        gains = gains + nbuf[k].astype(jnp.float32)
    lowbuf[x, z, y, :, ROWS : ROWS + 128] = gains.astype(jnp.bfloat16)

    def hop_copy(ref, slot, device):
        return pltpu.make_async_remote_copy(
            src_ref=ref, dst_ref=ref, send_sem=psend.at[slot], recv_sem=precv.at[slot],
            device_id=device, device_id_type=MESH,
        )

    along_z = [hop_copy(lowbuf.at[x, z, y], k - 1, {"z": lax.rem(z + k, Z)}) for k in range(1, Z)]
    along_y = [hop_copy(lowbuf.at[x, :, y], Z - 2 + k, {"y": lax.rem(y + k, Y)}) for k in range(1, Y)]
    along_x = [hop_copy(lowbuf.at[x], Z + Y - 3 + k, {"x": lax.rem(x + k, X)}) for k in range(1, X)]
    for copy in along_z:
        copy.start()
    send_blocks(5, 11)
    for copy in along_z:
        copy.wait()
    for copy in along_y:
        copy.start()
    send_blocks(11, 18)
    for copy in along_y:
        copy.wait()
    for copy in along_x:
        copy.start()
    send_blocks(18, PLANE)
    for copy in along_x:
        copy.wait()

    acc[...] = jnp.zeros_like(acc)

    def add_block(block, from_z, from_y):
        low = jnp.concatenate([lowbuf[k, from_z, from_y, :, 0:ROWS] for k in range(X)], axis=0)
        fresh = block.astype(jnp.float32) + mix_rate * jnp.dot(high_t, low, preferred_element_type=jnp.float32)
        from_row = from_z * Y + from_y
        fresh_ref[:, pl.ds(pl.multiple_of(from_row * ROWS, 128), ROWS)] = fresh
        square = fresh * fresh
        acc[...] += square[:, 0:128] + square[:, 128:256] + square[:, 256:384]

    add_block(stage[row], z, y)

    @pl.loop(0, PLANE)
    def _(r):
        norm_ref[pl.ds(r * 3, 3), :] = lowbuf[0, r // Y, lax.rem(r, Y), 0:16, ROWS : ROWS + 128].astype(jnp.float32)[0:3]

    @pl.loop(1, PLANE)
    def _(i):
        d = lax.rem(i * STRIDE, PLANE)
        block_copy(d).wait()
        add_block(recv[d], lax.rem(z - d // Y + Z, Z), lax.rem(y - lax.rem(d, Y) + Y, Y))

    scale = jnp.broadcast_to(jnp.sqrt(jnp.sum(acc[...], axis=1, keepdims=True)), (MINE, 128))
    inv_ref[...] = 1.0 / scale
    scale_ref[...] = jnp.concatenate([scale, jnp.zeros((64, 128), jnp.float32)], axis=0).T[0:8]


def scale_kernel(fresh_ref, inv_ref, serve_ref):
    width = serve_ref.shape[1]
    at = pl.program_id(0) * width
    inv = inv_ref[...]
    for k in range(width // 128):
        part = fresh_ref[:, pl.ds(pl.multiple_of(at + k * 128, 128), 128)]
        serve_ref[:, k * 128 : (k + 1) * 128] = (part * inv).astype(jnp.bfloat16)


def per_device(weight_up, low_up, high_up, norm_train, norm_step):
    vmem = pl.BlockSpec(memory_space=pltpu.VMEM)
    hbm = pl.BlockSpec(memory_space=pltpu.HBM)
    bf16, f32 = jnp.bfloat16, jnp.float32
    dma = pltpu.SemaphoreType.DMA
    operands = weight_up, low_up.T, high_up, norm_train.reshape(1, PIECE), norm_step.reshape(1, PIECE)
    fresh, inv, scale, norm = pl.pallas_call(
        comm_kernel,
        out_shape=(
            pltpu.VMEM((MINE, D_MODEL), f32),
            pltpu.VMEM((MINE, 128), f32),
            jax.ShapeDtypeStruct((8, 256), f32),
            jax.ShapeDtypeStruct((D_MODEL // 128, 128), f32),
        ),
        in_specs=[hbm] * 5,
        out_specs=(vmem, vmem, vmem, vmem),
        scratch_shapes=[
            pltpu.VMEM((PLANE // 2, ROWS, 2 * MINE), bf16),
            pltpu.VMEM((PLANE, MINE, ROWS), bf16),
            pltpu.VMEM((PLANE, MINE, ROWS), bf16),
            pltpu.VMEM((X, Z, Y, 16, ROWS + 128), bf16),
            pltpu.VMEM((X * C, 16, 128), bf16),
            pltpu.VMEM((RANK, 2 * MINE), bf16),
            pltpu.VMEM((2 * MINE, 128), f32),
            pltpu.VMEM((MINE, 128), f32),
            pltpu.VMEM((RANK, ROWS), bf16),
            pltpu.VMEM((1, PIECE), f32),
            pltpu.VMEM((1, PIECE), f32),
            dma((PLANE // 2,)), dma((4,)), dma((PLANE,)), dma((PLANE,)),
            dma((X * C,)), dma((X * C,)), dma((Z + Y + X - 3,)), dma((Z + Y + X - 3,)),
        ],
        compiler_params=pltpu.CompilerParams(
            collective_id=0, has_side_effects=True, vmem_limit_bytes=40 * 2**20
        ),
        name="exchange",
    )(*(pltpu.with_memory_space_constraint(a, pltpu.HBM) for a in operands))
    steps = 8
    serve_t = pl.pallas_call(
        scale_kernel,
        grid=(steps,),
        out_shape=jax.ShapeDtypeStruct((MINE, D_MODEL), bf16),
        in_specs=[vmem, vmem],
        out_specs=pl.BlockSpec((MINE, D_MODEL // steps), lambda i: (0, i)),
        compiler_params=pltpu.CompilerParams(vmem_limit_bytes=16 * 2**20),
        name="rescale",
    )(fresh, inv)
    return serve_t.T, scale[0, :MINE], norm.reshape(-1).astype(bf16)


def solution(mesh):
    split = Mesh(mesh.devices.reshape(Z, Y, X, C), ("z", "y", "x", "c"))
    rows, cols = ("z", "y"), ("x", "c")
    in_specs = (P(rows, cols), P(rows, None), P(None, cols), P(rows + cols), P(rows + cols))
    out_specs = (P(None, cols + rows), P(cols + rows), P())
    return jax.shard_map(per_device, mesh=split, in_specs=in_specs, out_specs=out_specs, check_vma=False)
```

```python
import functools

import jax
import jax.numpy as jnp
from jax import lax
from jax.experimental import pallas as pl
from jax.experimental.pallas import tpu as pltpu
from jax.sharding import Mesh
from jax.sharding import PartitionSpec as P

MESH = pl.DeviceIdType.MESH
Z, Y, X, C = 8, 4, 4, 2
PLANE = Z * Y
D_MODEL, RANK = 12288, 64
ROWS = D_MODEL // PLANE
COLS = 6144
MINE = COLS // PLANE
PIECE = D_MODEL // (PLANE * X * C)
STEPS = PLANE // 2
ORDER, START = 7, 7
AFTER_Z, AFTER_Y = 2, 2
WRITES = 2
HEAD = 4

mix_rate = 0.5


def comm_kernel(
    w_hbm, low_hbm, high_hbm, train_hbm, step_hbm,
    fresh_ref, inv_ref, scale_ref, norm_ref,
    wbuf, stage, recv, lowbuf, nbuf, hpair, ht, acc, norms, low_ref, nt_ref, ns_ref,
    wsem, isem, ssend, srecv, nsend, nrecv, psend, precv,
):
    z, y = lax.axis_index("z"), lax.axis_index("y")
    x, c = lax.axis_index("x"), lax.axis_index("c")
    row = z * Y + y
    me = x * C + c

    def step(s):
        t = lax.rem(s * ORDER + START, STEPS)
        return t // 2, lax.rem(t, 2)

    def partner(dz, q, j):
        return lax.rem(z + dz, Z), 2 * lax.rem(y // 2 + q, 2) + lax.rem(y + j, 2)

    def side_device(k):
        other = lax.rem(me + k, X * C)
        return {"x": other // C, "c": lax.rem(other, C)}

    def pair_of(s):
        dz, q = step(s)
        to_z, to_y = partner(dz, q, 0)
        return to_z * (Y // 2) + to_y // 2

    def weight_copy(s):
        return pltpu.make_async_copy(
            w_hbm.at[:, pl.ds(pl.multiple_of(pair_of(s) * 2 * MINE, 128), 2 * MINE)], wbuf.at[s], wsem.at[s]
        )

    for s in range(2):
        weight_copy(s).start()

    barrier = pltpu.get_barrier_semaphore()
    for t in range(1, PLANE):
        to_z, to_y = partner(t // Y, t % Y // 2, t % 2)
        pl.semaphore_signal(barrier, inc=1, device_id={"z": to_z, "y": to_y}, device_id_type=MESH)
    for k in range(1, X * C):
        pl.semaphore_signal(barrier, inc=1, device_id=side_device(k), device_id_type=MESH)

    for s in range(2, HEAD):
        weight_copy(s).start()
    pair = high_hbm.at[:, pl.ds(pl.multiple_of((row // 2) * 2 * MINE, 128), 2 * MINE)]
    small = [
        pltpu.make_async_copy(ref, to, isem.at[k])
        for k, (ref, to) in enumerate(((train_hbm, nt_ref), (step_hbm, ns_ref), (low_hbm, low_ref), (pair, hpair)))
    ]
    for copy in small:
        copy.start()
    for s in range(HEAD, STEPS):
        weight_copy(s).start()

    def turn(s):
        weight_copy(s).wait()
        turned = wbuf[s].T
        stage[2 * s] = turned[0:MINE]
        stage[2 * s + 1] = turned[MINE : 2 * MINE]

    def block_copy(s, j):
        dz, q = step(s)
        to_z, to_y = partner(dz, q, j)
        slot = dz * Y + 2 * q + j
        return pltpu.make_async_remote_copy(
            src_ref=stage.at[2 * s + lax.rem(to_y, 2)], dst_ref=recv.at[slot],
            send_sem=ssend.at[slot], recv_sem=srecv.at[slot],
            device_id={"z": to_z, "y": to_y}, device_id_type=MESH,
        )

    def send(s):
        dz, q = step(s)

        @pl.when(dz + q > 0)
        def _():
            block_copy(s, 0).start()

        block_copy(s, 1).start()

    @pl.loop(0, HEAD)
    def _(s):
        turn(s)

    for copy in small:
        copy.wait()
    gain = (nt_ref[...] + ns_ref[...]).astype(jnp.bfloat16).astype(jnp.float32)
    spot = me * PIECE + lax.broadcasted_iota(jnp.int32, (16, PIECE), 1)
    in_row = spot // 128 == lax.broadcasted_iota(jnp.int32, (16, PIECE), 0)
    left = jnp.where(in_row, jnp.broadcast_to(gain, (16, PIECE)), 0.0).astype(jnp.bfloat16)
    lane = lax.rem(me * PIECE + lax.broadcasted_iota(jnp.int32, (PIECE, 128), 0), 128)
    right = jnp.where(lane == lax.broadcasted_iota(jnp.int32, (PIECE, 128), 1), 1.0, 0.0).astype(jnp.bfloat16)
    nbuf[me] = jnp.dot(left, right, preferred_element_type=jnp.float32).astype(jnp.bfloat16)

    ranks = pl.ds(pl.multiple_of(x * 16, 16), 16)

    @pl.when(c == 0)
    def _():
        lowbuf[0, x, z, y] = low_ref[ranks, 0:256]

    @pl.when(c == 1)
    def _():
        lowbuf[1, x, z, y, :, 0:128] = low_ref[ranks, 256:384]

    pl.semaphore_wait(barrier, PLANE - 1 + X * C - 1)

    def gain_copy(k):
        return pltpu.make_async_remote_copy(
            src_ref=nbuf.at[me], dst_ref=nbuf.at[me], send_sem=nsend.at[k], recv_sem=nrecv.at[k],
            device_id=side_device(k), device_id_type=MESH,
        )

    for s in range(HEAD - 1):
        send(s)
    for k in range(1, X * C):
        gain_copy(k).start()

    def turn_and_send(first, last):
        @pl.loop(first, last)
        def _(s):
            turn(s)
            send(s - 1)

    turn_and_send(HEAD, HEAD + 3)
    for k in range(1, X * C):
        gain_copy(k).wait()
    gains = nbuf[0].astype(jnp.float32)
    for k in range(1, X * C):
        gains = gains + nbuf[k].astype(jnp.float32)

    @pl.when(c == 1)
    def _():
        lowbuf[1, x, z, y, :, 128:256] = gains.astype(jnp.bfloat16)

    def hop_copy(ref, slot, device):
        return pltpu.make_async_remote_copy(
            src_ref=ref, dst_ref=ref, send_sem=psend.at[slot], recv_sem=precv.at[slot],
            device_id=device, device_id_type=MESH,
        )

    along_z = [hop_copy(lowbuf.at[c, x, z, y], k - 1, {"z": lax.rem(z + k, Z)}) for k in range(1, Z)]
    along_y = [hop_copy(lowbuf.at[c, x, :, y], Z - 2 + k, {"y": lax.rem(y + k, Y)}) for k in range(1, Y)]
    aside = [hop_copy(lowbuf.at[c, x], Z + Y - 3 + k, side_device(k)) for k in range(1, X * C)]
    turn_and_send(HEAD + 3, HEAD + 4)
    for copy in along_z:
        copy.start()
    turn_and_send(HEAD + 4, STEPS - AFTER_Z - AFTER_Y)

    @pl.loop(STEPS - AFTER_Z - AFTER_Y, STEPS)
    def _(s):
        turn(s)

    for copy in along_z:
        copy.wait()
    for copy in along_y:
        copy.start()
    for s in range(STEPS - AFTER_Z - AFTER_Y - 1, STEPS - AFTER_Y - 1):
        send(s)
    for copy in along_y:
        copy.wait()
    for copy in aside:
        copy.start()
    for s in range(STEPS - AFTER_Y - 1, STEPS):
        send(s)

    wide = jnp.concatenate([hpair[...].astype(jnp.float32), jnp.zeros((RANK, 2 * MINE), jnp.float32)], axis=0)
    ht[...] = wide.T
    mine = pl.ds(pl.multiple_of(lax.rem(row, 2) * MINE, 8), MINE)
    high_t = ht[mine, :][:, 0:RANK].astype(jnp.bfloat16)

    for copy in aside:
        copy.wait()

    acc[...] = jnp.zeros_like(acc)

    def add_block(block, from_z, from_y):
        low = jnp.concatenate(
            [
                jnp.concatenate([lowbuf[0, k, from_z, from_y], lowbuf[1, k, from_z, from_y, :, 0:128]], axis=1)
                for k in range(X)
            ],
            axis=0,
        )
        fresh = block.astype(jnp.float32) + mix_rate * jnp.dot(high_t, low, preferred_element_type=jnp.float32)
        from_row = from_z * Y + from_y
        fresh_ref[:, pl.ds(pl.multiple_of(from_row * ROWS, 128), ROWS)] = fresh
        square = fresh * fresh
        acc[...] += square[:, 0:128] + square[:, 128:256] + square[:, 256:384]

    @pl.loop(0, PLANE)
    def _(r):
        norms[pl.ds(r * 3, 3), :] = lowbuf[1, 0, r // Y, lax.rem(r, Y), :, 128:256].astype(jnp.float32)[0:3]

    norm_ref[...] = norms[...].astype(jnp.bfloat16)

    @pl.loop(0, STEPS)
    def _(s):
        dz, q = step(s)

        @pl.loop(0, 2)
        def _(j):
            away = dz + q + j > 0
            from_z = lax.rem(z + Z - dz, Z)
            from_y = partner(dz, q, j)[1]

            @pl.when(away)
            def _():
                block_copy(s, j).wait()
                add_block(recv[dz * Y + 2 * q + j], from_z, from_y)

            @pl.when(jnp.logical_not(away))
            def _():
                add_block(stage[2 * s + lax.rem(y, 2)], z, y)

    scale = jnp.broadcast_to(jnp.sqrt(jnp.sum(acc[...], axis=1, keepdims=True)), (MINE, 128))
    inv_ref[...] = 1.0 / scale
    scale_ref[...] = jnp.concatenate([scale, jnp.zeros((64, 128), jnp.float32)], axis=0).T[0:8]


def scale_kernel(fresh_ref, inv_ref, scale_ref, norm_ref, serve_ref, scale_out, norm_out):
    width = serve_ref.shape[1]
    at = pl.program_id(0) * width
    inv = inv_ref[...]
    for k in range(width // 128):
        part = fresh_ref[:, pl.ds(pl.multiple_of(at + k * 128, 128), 128)]
        serve_ref[:, k * 128 : (k + 1) * 128] = (part * inv).astype(jnp.bfloat16)

    @pl.when(pl.program_id(0) == 0)
    def _():
        scale_out[...] = scale_ref[0:1, 0:MINE]
        norm_out[...] = norm_ref[...]


def per_device(weight_up, low_up, high_up, norm_train, norm_step):
    vmem = pl.BlockSpec(memory_space=pltpu.VMEM)
    hbm = pl.BlockSpec(memory_space=pltpu.HBM)
    bf16, f32 = jnp.bfloat16, jnp.float32
    dma = pltpu.SemaphoreType.DMA
    operands = weight_up, low_up.T, high_up, norm_train.reshape(1, PIECE), norm_step.reshape(1, PIECE)
    hops = Z + Y + X * C - 3
    found = pl.pallas_call(
        comm_kernel,
        out_shape=(
            pltpu.VMEM((MINE, D_MODEL), f32),
            pltpu.VMEM((MINE, 128), f32),
            pltpu.VMEM((8, 256), f32),
            pltpu.VMEM((D_MODEL // 128, 128), bf16),
        ),
        in_specs=[hbm] * 5,
        out_specs=(vmem, vmem, vmem, vmem),
        scratch_shapes=[
            pltpu.VMEM((STEPS, ROWS, 2 * MINE), bf16),
            pltpu.VMEM((PLANE, MINE, ROWS), bf16),
            pltpu.VMEM((PLANE, MINE, ROWS), bf16),
            pltpu.VMEM((C, X, Z, Y, 16, 256), bf16),
            pltpu.VMEM((X * C, 16, 128), bf16),
            pltpu.VMEM((RANK, 2 * MINE), bf16),
            pltpu.VMEM((2 * MINE, 128), f32),
            pltpu.VMEM((MINE, 128), f32),
            pltpu.VMEM((D_MODEL // 128, 128), f32),
            pltpu.VMEM((RANK, ROWS), bf16),
            pltpu.VMEM((1, PIECE), f32),
            pltpu.VMEM((1, PIECE), f32),
            dma((STEPS,)), dma((4,)), dma((PLANE,)), dma((PLANE,)),
            dma((X * C,)), dma((X * C,)), dma((hops,)), dma((hops,)),
        ],
        compiler_params=pltpu.CompilerParams(
            collective_id=0, has_side_effects=True, vmem_limit_bytes=40 * 2**20
        ),
        name="exchange",
    )(*(pltpu.with_memory_space_constraint(a, pltpu.HBM) for a in operands))
    serve_t, scale, norm = pl.pallas_call(
        scale_kernel,
        grid=(WRITES,),
        out_shape=(
            jax.ShapeDtypeStruct((MINE, D_MODEL), bf16),
            jax.ShapeDtypeStruct((1, MINE), f32),
            jax.ShapeDtypeStruct((D_MODEL // 128, 128), bf16),
        ),
        in_specs=[vmem] * 4,
        out_specs=(
            pl.BlockSpec((MINE, D_MODEL // WRITES), lambda i: (0, i)),
            pl.BlockSpec((1, MINE), lambda i: (0, 0)),
            pl.BlockSpec((D_MODEL // 128, 128), lambda i: (0, 0)),
        ),
        compiler_params=pltpu.CompilerParams(vmem_limit_bytes=12 * 2**20),
        name="rescale",
    )(*found)
    return serve_t.T, scale.reshape(-1), norm.reshape(-1)


def solution(mesh):
    split = Mesh(mesh.devices.reshape(Z, Y, X, C), ("z", "y", "x", "c"))
    rows, cols = ("z", "y"), ("x", "c")
    in_specs = (P(rows, cols), P(rows, None), P(None, cols), P(rows + cols), P(rows + cols))
    out_specs = (P(None, cols + rows), P(cols + rows), P())
    return jax.shard_map(per_device, mesh=split, in_specs=in_specs, out_specs=out_specs, check_vma=False)
```

```python
import functools

import jax
import jax.numpy as jnp
from jax import lax
from jax.experimental import pallas as pl
from jax.experimental.pallas import tpu as pltpu
from jax.sharding import Mesh
from jax.sharding import PartitionSpec as P

MESH = pl.DeviceIdType.MESH
Z, Y, X, C = 8, 4, 4, 2
PLANE = Z * Y
D_MODEL, RANK = 12288, 64
ROWS = D_MODEL // PLANE
COLS = 6144
MINE = COLS // PLANE
PIECE = D_MODEL // (PLANE * X * C)
STEPS = PLANE // 2
WRITES = 2

mix_rate = 0.5


def comm_kernel(
    w_hbm, low_hbm, high_hbm, train_hbm, step_hbm,
    fresh_ref, inv_ref, scale_ref, norm_ref,
    wbuf, stage, recv, relay, lowbuf, nbuf, hpair, ht, acc, norms, low_ref, nt_ref, ns_ref,
    wsem, isem, zsend, zrecv, ysend, yrecv, nsend, nrecv, psend, precv,
):
    z, y = lax.axis_index("z"), lax.axis_index("y")
    x, c = lax.axis_index("x"), lax.axis_index("c")
    row = z * Y + y
    me = x * C + c

    def step(s):
        return away(lax.rem(s, Z)), 1 - s // Z

    def step_of(dz, q):
        k = lax.rem(dz + Z - 1, Z)
        return 2 * lax.rem(k, Z // 2) + k // (Z // 2) + (1 - q) * Z

    def away(k):
        return lax.rem(1 + k // 2 + Z // 2 * lax.rem(k, 2), Z)

    def partner(dz, q, j):
        return lax.rem(z + dz, Z), 2 * lax.rem(y // 2 + q, 2) + lax.rem(y + j, 2)

    def side_device(k):
        other = lax.rem(me + k, X * C)
        return {"x": other // C, "c": lax.rem(other, C)}

    def pair_of(s):
        dz, q = step(s)
        to_z, to_y = partner(dz, q, 0)
        return to_z * (Y // 2) + to_y // 2

    def weight_copy(s):
        return pltpu.make_async_copy(
            w_hbm.at[:, pl.ds(pl.multiple_of(pair_of(s) * 2 * MINE, 128), 2 * MINE)], wbuf.at[s], wsem.at[s]
        )

    for s in range(2):
        weight_copy(s).start()

    barrier = pltpu.get_barrier_semaphore()
    for k in range(1, Z):
        pl.semaphore_signal(barrier, inc=1, device_id={"z": lax.rem(z + k, Z)}, device_id_type=MESH)
    for k in range(1, Y):
        pl.semaphore_signal(barrier, inc=1, device_id={"y": lax.rem(y + k, Y)}, device_id_type=MESH)
    for k in range(1, X * C):
        pl.semaphore_signal(barrier, inc=1, device_id=side_device(k), device_id_type=MESH)

    pair = high_hbm.at[:, pl.ds(pl.multiple_of((row // 2) * 2 * MINE, 128), 2 * MINE)]
    small = [
        pltpu.make_async_copy(ref, to, isem.at[k])
        for k, (ref, to) in enumerate(((train_hbm, nt_ref), (step_hbm, ns_ref), (low_hbm, low_ref), (pair, hpair)))
    ]
    for copy in small:
        copy.start()
    for s in range(2, STEPS):
        weight_copy(s).start()

    def turn(s):
        weight_copy(s).wait()
        turned = wbuf[s].T
        stage[2 * s] = turned[0:MINE]
        stage[2 * s + 1] = turned[MINE : 2 * MINE]

    def copy_z(dz, e, into):
        q, j = e // 2, lax.rem(e, 2)
        to_z, to_y = partner(dz, q, j)
        slot = dz * Y + e
        return pltpu.make_async_remote_copy(
            src_ref=stage.at[2 * step_of(dz, q) + lax.rem(to_y, 2)], dst_ref=into.at[slot],
            send_sem=zsend.at[slot], recv_sem=zrecv.at[slot], device_id={"z": to_z}, device_id_type=MESH,
        )

    def copy_y(ref, dz, e):
        slot = dz * Y + e
        return pltpu.make_async_remote_copy(
            src_ref=ref, dst_ref=recv.at[slot], send_sem=ysend.at[slot], recv_sem=yrecv.at[slot],
            device_id={"y": partner(dz, e // 2, lax.rem(e, 2))[1]}, device_id_type=MESH,
        )

    def each(first, last, do):
        @pl.loop(first, last)
        def _(k):
            do(k)

    def turn_and_send(first, last, e):
        @pl.loop(first, last)
        def _(s):
            turn(s)
            copy_z(step(s - 1)[0], e, relay).start()

    turn(0)
    turn(1)
    pl.semaphore_wait(barrier, Z - 1 + Y - 1 + X * C - 1)
    copy_z(1, 2, relay).start()

    for copy in small:
        copy.wait()
    gain = (nt_ref[...] + ns_ref[...]).astype(jnp.bfloat16).astype(jnp.float32)
    spot = me * PIECE + lax.broadcasted_iota(jnp.int32, (16, PIECE), 1)
    in_row = spot // 128 == lax.broadcasted_iota(jnp.int32, (16, PIECE), 0)
    left = jnp.where(in_row, jnp.broadcast_to(gain, (16, PIECE)), 0.0).astype(jnp.bfloat16)
    lane = lax.rem(me * PIECE + lax.broadcasted_iota(jnp.int32, (PIECE, 128), 0), 128)
    right = jnp.where(lane == lax.broadcasted_iota(jnp.int32, (PIECE, 128), 1), 1.0, 0.0).astype(jnp.bfloat16)
    nbuf[me] = jnp.dot(left, right, preferred_element_type=jnp.float32).astype(jnp.bfloat16)

    ranks = pl.ds(pl.multiple_of(x * 16, 16), 16)

    @pl.when(c == 0)
    def _():
        lowbuf[0, x, z, y] = low_ref[ranks, 0:256]

    @pl.when(c == 1)
    def _():
        lowbuf[1, x, z, y, :, 0:128] = low_ref[ranks, 256:384]

    def gain_copy(k):
        return pltpu.make_async_remote_copy(
            src_ref=nbuf.at[me], dst_ref=nbuf.at[me], send_sem=nsend.at[k], recv_sem=nrecv.at[k],
            device_id=side_device(k), device_id_type=MESH,
        )

    for k in range(1, X * C):
        gain_copy(k).start()
    turn_and_send(2, Z, 2)
    for k in range(1, X * C):
        gain_copy(k).wait()
    gains = nbuf[0].astype(jnp.float32)
    for k in range(1, X * C):
        gains = gains + nbuf[k].astype(jnp.float32)

    @pl.when(c == 1)
    def _():
        lowbuf[1, x, z, y, :, 128:256] = gains.astype(jnp.bfloat16)

    def hop_copy(ref, slot, device):
        return pltpu.make_async_remote_copy(
            src_ref=ref, dst_ref=ref, send_sem=psend.at[slot], recv_sem=precv.at[slot],
            device_id=device, device_id_type=MESH,
        )

    along_z = [hop_copy(lowbuf.at[c, x, z, y], k - 1, {"z": lax.rem(z + k, Z)}) for k in range(1, Z)]
    along_y = [hop_copy(lowbuf.at[c, x, :, y], Z - 2 + k, {"y": lax.rem(y + k, Y)}) for k in range(1, Y)]
    aside = [hop_copy(lowbuf.at[c, x], Z + Y - 3 + k, side_device(k)) for k in range(1, X * C)]
    for copy in along_z:
        copy.start()
    each(0, Z - 1, lambda k: copy_z(away(k), 3, relay).start())
    beside = [copy_y(stage.at[2 * step_of(0, e // 2) + lax.rem(y + e % 2, 2)], 0, e) for e in range(1, Y)]
    for copy in beside[1:]:
        copy.start()
    turn(Z)
    turn_and_send(Z + 1, STEPS, 1)
    each(0, Z - 1, lambda k: copy_z(away(k), 0, recv).start())
    beside[0].start()

    wide = jnp.concatenate([hpair[...].astype(jnp.float32), jnp.zeros((RANK, 2 * MINE), jnp.float32)], axis=0)
    ht[...] = wide.T
    mine = pl.ds(pl.multiple_of(lax.rem(row, 2) * MINE, 8), MINE)
    high_t = ht[mine, :][:, 0:RANK].astype(jnp.bfloat16)

    for copy in along_z:
        copy.wait()
    for copy in along_y:
        copy.start()

    def pass_on(dz, e):
        copy_z(dz, e, relay).wait_recv()
        copy_y(relay.at[dz * Y + e], dz, e).start()

    each(0, Z - 1, lambda k: pass_on(away(k), 2))
    for copy in along_y:
        copy.wait()
    for copy in aside:
        copy.start()
    each(0, Z - 1, lambda k: pass_on(away(k), 3))
    for copy in aside:
        copy.wait()

    acc[...] = jnp.zeros_like(acc)

    def add_block(block, from_z, from_y):
        low = jnp.concatenate(
            [
                jnp.concatenate([lowbuf[0, k, from_z, from_y], lowbuf[1, k, from_z, from_y, :, 0:128]], axis=1)
                for k in range(X)
            ],
            axis=0,
        )
        fresh = block.astype(jnp.float32) + mix_rate * jnp.dot(high_t, low, preferred_element_type=jnp.float32)
        from_row = from_z * Y + from_y
        fresh_ref[:, pl.ds(pl.multiple_of(from_row * ROWS, 128), ROWS)] = fresh
        square = fresh * fresh
        acc[...] += square[:, 0:128] + square[:, 128:256] + square[:, 256:384]

    @pl.loop(0, PLANE)
    def _(r):
        norms[pl.ds(r * 3, 3), :] = lowbuf[1, 0, r // Y, lax.rem(r, Y), :, 128:256].astype(jnp.float32)[0:3]

    norm_ref[...] = norms[...].astype(jnp.bfloat16)

    def add_from(dz, e):
        add_block(recv[dz * Y + e], lax.rem(z + Z - dz, Z), partner(dz, e // 2, lax.rem(e, 2))[1])

    def add_passed(dz, e):
        copy_y(relay.at[dz * Y + e], dz, e).wait_recv()
        add_from(dz, e)

    def pass_and_add(k):
        dz = away(k)
        pass_on(dz, 1)
        add_passed(dz, 2)
        add_passed(dz, 3)

    def add_last(k):
        dz = away(k)
        copy_z(dz, 0, recv).wait_recv()
        add_from(dz, 0)

    add_block(stage[2 * step_of(0, 0) + lax.rem(y, 2)], z, y)
    each(1, Y, lambda e: add_passed(0, e))
    each(0, Z - 1, pass_and_add)
    each(0, Z - 1, lambda k: add_passed(away(k), 1))
    each(0, Z - 1, add_last)

    def sent_z(slot):
        copy_z(slot // Y, lax.rem(slot, Y), recv).wait_send()

    def sent_y(slot):
        @pl.when(lax.rem(slot, Y) > 0)
        def _():
            copy_y(relay.at[slot], slot // Y, lax.rem(slot, Y)).wait_send()

    each(Y, PLANE, sent_z)
    each(0, PLANE, sent_y)

    scale = jnp.broadcast_to(jnp.sqrt(jnp.sum(acc[...], axis=1, keepdims=True)), (MINE, 128))
    inv_ref[...] = 1.0 / scale
    scale_ref[...] = jnp.concatenate([scale, jnp.zeros((64, 128), jnp.float32)], axis=0).T[0:8]


def scale_kernel(fresh_ref, inv_ref, scale_ref, norm_ref, serve_ref, scale_out, norm_out):
    width = serve_ref.shape[1]
    at = pl.program_id(0) * width
    inv = inv_ref[...]
    for k in range(width // 128):
        part = fresh_ref[:, pl.ds(pl.multiple_of(at + k * 128, 128), 128)]
        serve_ref[:, k * 128 : (k + 1) * 128] = (part * inv).astype(jnp.bfloat16)

    @pl.when(pl.program_id(0) == 0)
    def _():
        scale_out[...] = scale_ref[0:1, 0:MINE]
        norm_out[...] = norm_ref[...]


def per_device(weight_up, low_up, high_up, norm_train, norm_step):
    vmem = pl.BlockSpec(memory_space=pltpu.VMEM)
    hbm = pl.BlockSpec(memory_space=pltpu.HBM)
    bf16, f32 = jnp.bfloat16, jnp.float32
    dma = pltpu.SemaphoreType.DMA
    operands = weight_up, low_up.T, high_up, norm_train.reshape(1, PIECE), norm_step.reshape(1, PIECE)
    hops = Z + Y + X * C - 3
    found = pl.pallas_call(
        comm_kernel,
        out_shape=(
            pltpu.VMEM((MINE, D_MODEL), f32),
            pltpu.VMEM((MINE, 128), f32),
            pltpu.VMEM((8, 256), f32),
            pltpu.VMEM((D_MODEL // 128, 128), bf16),
        ),
        in_specs=[hbm] * 5,
        out_specs=(vmem, vmem, vmem, vmem),
        scratch_shapes=[
            pltpu.VMEM((STEPS, ROWS, 2 * MINE), bf16),
            pltpu.VMEM((PLANE, MINE, ROWS), bf16),
            pltpu.VMEM((PLANE, MINE, ROWS), bf16),
            pltpu.VMEM((PLANE, MINE, ROWS), bf16),
            pltpu.VMEM((C, X, Z, Y, 16, 256), bf16),
            pltpu.VMEM((X * C, 16, 128), bf16),
            pltpu.VMEM((RANK, 2 * MINE), bf16),
            pltpu.VMEM((2 * MINE, 128), f32),
            pltpu.VMEM((MINE, 128), f32),
            pltpu.VMEM((D_MODEL // 128, 128), f32),
            pltpu.VMEM((RANK, ROWS), bf16),
            pltpu.VMEM((1, PIECE), f32),
            pltpu.VMEM((1, PIECE), f32),
            dma((STEPS,)), dma((4,)), dma((PLANE,)), dma((PLANE,)), dma((PLANE,)), dma((PLANE,)),
            dma((X * C,)), dma((X * C,)), dma((hops,)), dma((hops,)),
        ],
        compiler_params=pltpu.CompilerParams(
            collective_id=0, has_side_effects=True, vmem_limit_bytes=40 * 2**20
        ),
        name="exchange",
    )(*(pltpu.with_memory_space_constraint(a, pltpu.HBM) for a in operands))
    serve_t, scale, norm = pl.pallas_call(
        scale_kernel,
        grid=(WRITES,),
        out_shape=(
            jax.ShapeDtypeStruct((MINE, D_MODEL), bf16),
            jax.ShapeDtypeStruct((1, MINE), f32),
            jax.ShapeDtypeStruct((D_MODEL // 128, 128), bf16),
        ),
        in_specs=[vmem] * 4,
        out_specs=(
            pl.BlockSpec((MINE, D_MODEL // WRITES), lambda i: (0, i)),
            pl.BlockSpec((1, MINE), lambda i: (0, 0)),
            pl.BlockSpec((D_MODEL // 128, 128), lambda i: (0, 0)),
        ),
        compiler_params=pltpu.CompilerParams(vmem_limit_bytes=12 * 2**20),
        name="rescale",
    )(*found)
    return serve_t.T, scale.reshape(-1), norm.reshape(-1)


def solution(mesh):
    split = Mesh(mesh.devices.reshape(Z, Y, X, C), ("z", "y", "x", "c"))
    rows, cols = ("z", "y"), ("x", "c")
    in_specs = (P(rows, cols), P(rows, None), P(None, cols), P(rows + cols), P(rows + cols))
    out_specs = (P(None, cols + rows), P(cols + rows), P())
    return jax.shard_map(per_device, mesh=split, in_specs=in_specs, out_specs=out_specs, check_vma=False)
```

```python
import functools

import jax
import jax.numpy as jnp
from jax import lax
from jax.experimental import pallas as pl
from jax.experimental.pallas import tpu as pltpu
from jax.sharding import Mesh
from jax.sharding import PartitionSpec as P

MESH = pl.DeviceIdType.MESH
Z, Y, X, C = 8, 4, 4, 2
PLANE = Z * Y
D_MODEL, RANK = 12288, 64
ROWS = D_MODEL // PLANE
COLS = 6144
MINE = COLS // PLANE
PIECE = D_MODEL // (PLANE * X * C)
STEPS = PLANE // 2
AWAY = (5, 1, 6, 2, 7, 3, 4, 0)
NEAR_FIRST = (7, 1, 6, 2, 5, 3, 4, 0)
WRITES = 2

mix_rate = 0.5


def comm_kernel(
    w_hbm, low_hbm, high_hbm, train_hbm, step_hbm,
    fresh_ref, inv_ref, scale_ref, norm_ref,
    wbuf, stage, recv, relay, lowbuf, nbuf, hpair, ht, acc, norms, low_ref, nt_ref, ns_ref,
    wsem, isem, zsend, zrecv, ysend, yrecv, nsend, nrecv, psend, precv,
):
    z, y = lax.axis_index("z"), lax.axis_index("y")
    x, c = lax.axis_index("x"), lax.axis_index("c")
    row = z * Y + y
    me = x * C + c

    def step(s):
        return away(s % Z if isinstance(s, int) else lax.rem(s, Z)), 1 - s // Z

    def step_of(dz, q):
        return listed(dz, [AWAY.index(k) for k in range(Z)]) + (1 - q) * Z

    def away(k):
        return listed(k, AWAY)

    def listed(k, table):
        if isinstance(k, int):
            return table[k]
        found = jnp.int32(table[0])
        for n in range(1, Z):
            found = jnp.where(k == n, table[n], found)
        return found

    def partner(dz, q, j):
        return lax.rem(z + dz, Z), 2 * lax.rem(y // 2 + q, 2) + lax.rem(y + j, 2)

    def side_device(k):
        other = lax.rem(me + k, X * C)
        return {"x": other // C, "c": lax.rem(other, C)}

    def pair_of(s):
        dz, q = step(s)
        to_z, to_y = partner(dz, q, 0)
        return to_z * (Y // 2) + to_y // 2

    def weight_copy(s):
        return pltpu.make_async_copy(
            w_hbm.at[:, pl.ds(pl.multiple_of(pair_of(s) * 2 * MINE, 128), 2 * MINE)], wbuf.at[s], wsem.at[s]
        )

    for s in range(2):
        weight_copy(s).start()

    barrier = pltpu.get_barrier_semaphore()
    for k in range(1, Z):
        pl.semaphore_signal(barrier, inc=1, device_id={"z": lax.rem(z + k, Z)}, device_id_type=MESH)
    for k in range(1, Y):
        pl.semaphore_signal(barrier, inc=1, device_id={"y": lax.rem(y + k, Y)}, device_id_type=MESH)
    for k in range(1, X * C):
        pl.semaphore_signal(barrier, inc=1, device_id=side_device(k), device_id_type=MESH)

    pair = high_hbm.at[:, pl.ds(pl.multiple_of((row // 2) * 2 * MINE, 128), 2 * MINE)]
    small = [
        pltpu.make_async_copy(ref, to, isem.at[k])
        for k, (ref, to) in enumerate(((train_hbm, nt_ref), (step_hbm, ns_ref), (low_hbm, low_ref), (pair, hpair)))
    ]
    for copy in small:
        copy.start()
    for s in range(2, STEPS):
        weight_copy(s).start()

    def turn(s):
        weight_copy(s).wait()
        turned = wbuf[s].T
        stage[2 * s] = turned[0:MINE]
        stage[2 * s + 1] = turned[MINE : 2 * MINE]

    def copy_z(dz, e, into):
        q, j = e // 2, lax.rem(e, 2)
        to_z, to_y = partner(dz, q, j)
        slot = dz * Y + e
        return pltpu.make_async_remote_copy(
            src_ref=stage.at[2 * step_of(dz, q) + lax.rem(to_y, 2)], dst_ref=into.at[slot],
            send_sem=zsend.at[slot], recv_sem=zrecv.at[slot], device_id={"z": to_z}, device_id_type=MESH,
        )

    def copy_y(ref, dz, e):
        slot = dz * Y + e
        return pltpu.make_async_remote_copy(
            src_ref=ref, dst_ref=recv.at[slot], send_sem=ysend.at[slot], recv_sem=yrecv.at[slot],
            device_id={"y": partner(dz, e // 2, lax.rem(e, 2))[1]}, device_id_type=MESH,
        )

    def each(first, last, do):
        @pl.loop(first, last)
        def _(k):
            do(k)

    def turn_and_send(first, last, e):
        @pl.loop(first, last)
        def _(s):
            turn(s)
            copy_z(step(s - 1)[0], e, relay).start()

    turn(0)
    turn(1)
    pl.semaphore_wait(barrier, Z - 1 + Y - 1 + X * C - 1)
    copy_z(away(0), 2, relay).start()
    turn_and_send(2, 4, 2)

    for copy in small:
        copy.wait()
    gain = (nt_ref[...] + ns_ref[...]).astype(jnp.bfloat16).astype(jnp.float32)
    spot = me * PIECE + lax.broadcasted_iota(jnp.int32, (16, PIECE), 1)
    in_row = spot // 128 == lax.broadcasted_iota(jnp.int32, (16, PIECE), 0)
    left = jnp.where(in_row, jnp.broadcast_to(gain, (16, PIECE)), 0.0).astype(jnp.bfloat16)
    lane = lax.rem(me * PIECE + lax.broadcasted_iota(jnp.int32, (PIECE, 128), 0), 128)
    right = jnp.where(lane == lax.broadcasted_iota(jnp.int32, (PIECE, 128), 1), 1.0, 0.0).astype(jnp.bfloat16)
    nbuf[me] = jnp.dot(left, right, preferred_element_type=jnp.float32).astype(jnp.bfloat16)

    ranks = pl.ds(pl.multiple_of(x * 16, 16), 16)

    @pl.when(c == 0)
    def _():
        lowbuf[0, x, z, y] = low_ref[ranks, 0:256]

    @pl.when(c == 1)
    def _():
        lowbuf[1, x, z, y, :, 0:128] = low_ref[ranks, 256:384]

    def gain_copy(k):
        return pltpu.make_async_remote_copy(
            src_ref=nbuf.at[me], dst_ref=nbuf.at[me], send_sem=nsend.at[k], recv_sem=nrecv.at[k],
            device_id=side_device(k), device_id_type=MESH,
        )

    for k in range(1, X * C):
        gain_copy(k).start()
    turn_and_send(4, Z, 2)
    for k in range(1, X * C):
        gain_copy(k).wait()
    gains = nbuf[0].astype(jnp.float32)
    for k in range(1, X * C):
        gains = gains + nbuf[k].astype(jnp.float32)

    @pl.when(c == 1)
    def _():
        lowbuf[1, x, z, y, :, 128:256] = gains.astype(jnp.bfloat16)

    def hop_copy(ref, slot, device):
        return pltpu.make_async_remote_copy(
            src_ref=ref, dst_ref=ref, send_sem=psend.at[slot], recv_sem=precv.at[slot],
            device_id=device, device_id_type=MESH,
        )

    along_z = [hop_copy(lowbuf.at[c, x, z, y], k - 1, {"z": lax.rem(z + k, Z)}) for k in range(1, Z)]
    along_y = [hop_copy(lowbuf.at[c, x, :, y], Z - 2 + k, {"y": lax.rem(y + k, Y)}) for k in range(1, Y)]
    aside = [hop_copy(lowbuf.at[c, x], Z + Y - 3 + k, side_device(k)) for k in range(1, X * C)]
    for copy in along_z:
        copy.start()
    each(0, Z - 1, lambda k: copy_z(away(k), 3, relay).start())
    beside = [copy_y(stage.at[2 * step_of(0, e // 2) + lax.rem(y + e % 2, 2)], 0, e) for e in range(1, Y)]
    for copy in beside[1:]:
        copy.start()
    turn(Z)
    turn_and_send(Z + 1, STEPS, 1)
    def last_away(k):
        return jnp.where(lax.rem(z + 1, Z) <= Z // 2, listed(k, NEAR_FIRST), listed(Z - 2 - k, NEAR_FIRST))

    each(0, Z - 1, lambda k: copy_z(last_away(k), 0, recv).start())
    beside[0].start()

    wide = jnp.concatenate([hpair[...].astype(jnp.float32), jnp.zeros((RANK, 2 * MINE), jnp.float32)], axis=0)
    ht[...] = wide.T
    mine = pl.ds(pl.multiple_of(lax.rem(row, 2) * MINE, 8), MINE)
    high_t = ht[mine, :][:, 0:RANK].astype(jnp.bfloat16)

    for copy in along_z:
        copy.wait()
    for copy in along_y:
        copy.start()

    def pass_on(dz, e):
        copy_z(dz, e, relay).wait_recv()
        copy_y(relay.at[dz * Y + e], dz, e).start()

    each(0, Z - 1, lambda k: pass_on(away(k), 2))
    for copy in along_y:
        copy.wait()
    for copy in aside:
        copy.start()
    each(0, Z - 1, lambda k: pass_on(away(k), 3))
    for copy in aside:
        copy.wait()

    acc[...] = jnp.zeros_like(acc)

    def add_block(block, from_z, from_y):
        low = jnp.concatenate(
            [
                jnp.concatenate([lowbuf[0, k, from_z, from_y], lowbuf[1, k, from_z, from_y, :, 0:128]], axis=1)
                for k in range(X)
            ],
            axis=0,
        )
        fresh = block.astype(jnp.float32) + mix_rate * jnp.dot(high_t, low, preferred_element_type=jnp.float32)
        from_row = from_z * Y + from_y
        fresh_ref[:, pl.ds(pl.multiple_of(from_row * ROWS, 128), ROWS)] = fresh
        square = fresh * fresh
        acc[...] += square[:, 0:128] + square[:, 128:256] + square[:, 256:384]

    @pl.loop(0, PLANE)
    def _(r):
        norms[pl.ds(r * 3, 3), :] = lowbuf[1, 0, r // Y, lax.rem(r, Y), :, 128:256].astype(jnp.float32)[0:3]

    norm_ref[...] = norms[...].astype(jnp.bfloat16)

    def add_from(dz, e):
        add_block(recv[dz * Y + e], lax.rem(z + Z - dz, Z), partner(dz, e // 2, lax.rem(e, 2))[1])

    def add_passed(dz, e):
        copy_y(relay.at[dz * Y + e], dz, e).wait_recv()
        add_from(dz, e)

    def pass_and_add(k):
        dz = away(k)
        pass_on(dz, 1)
        add_passed(dz, 2)
        add_passed(dz, 3)

    def add_last(k):
        dz = away(k)
        copy_z(dz, 0, recv).wait_recv()
        add_from(dz, 0)

    add_block(stage[2 * step_of(0, 0) + lax.rem(y, 2)], z, y)
    each(1, Y, lambda e: add_passed(0, e))
    each(0, Z - 1, pass_and_add)
    each(0, Z - 1, lambda k: add_passed(away(k), 1))
    each(0, Z - 1, add_last)

    def sent_z(slot):
        copy_z(slot // Y, lax.rem(slot, Y), recv).wait_send()

    def sent_y(slot):
        @pl.when(lax.rem(slot, Y) > 0)
        def _():
            copy_y(relay.at[slot], slot // Y, lax.rem(slot, Y)).wait_send()

    each(Y, PLANE, sent_z)
    each(0, PLANE, sent_y)

    scale = jnp.broadcast_to(jnp.sqrt(jnp.sum(acc[...], axis=1, keepdims=True)), (MINE, 128))
    inv_ref[...] = 1.0 / scale
    scale_ref[...] = jnp.concatenate([scale, jnp.zeros((64, 128), jnp.float32)], axis=0).T[0:8]


def scale_kernel(fresh_ref, inv_ref, scale_ref, norm_ref, serve_ref, scale_out, norm_out):
    width = serve_ref.shape[1]
    at = pl.program_id(0) * width
    inv = inv_ref[...]
    for k in range(width // 128):
        part = fresh_ref[:, pl.ds(pl.multiple_of(at + k * 128, 128), 128)]
        serve_ref[:, k * 128 : (k + 1) * 128] = (part * inv).astype(jnp.bfloat16)

    @pl.when(pl.program_id(0) == 0)
    def _():
        scale_out[...] = scale_ref[0:1, 0:MINE]
        norm_out[...] = norm_ref[...]


def per_device(weight_up, low_up, high_up, norm_train, norm_step):
    vmem = pl.BlockSpec(memory_space=pltpu.VMEM)
    hbm = pl.BlockSpec(memory_space=pltpu.HBM)
    bf16, f32 = jnp.bfloat16, jnp.float32
    dma = pltpu.SemaphoreType.DMA
    operands = weight_up, low_up.T, high_up, norm_train.reshape(1, PIECE), norm_step.reshape(1, PIECE)
    hops = Z + Y + X * C - 3
    found = pl.pallas_call(
        comm_kernel,
        out_shape=(
            pltpu.VMEM((MINE, D_MODEL), f32),
            pltpu.VMEM((MINE, 128), f32),
            pltpu.VMEM((8, 256), f32),
            pltpu.VMEM((D_MODEL // 128, 128), bf16),
        ),
        in_specs=[hbm] * 5,
        out_specs=(vmem, vmem, vmem, vmem),
        scratch_shapes=[
            pltpu.VMEM((STEPS, ROWS, 2 * MINE), bf16),
            pltpu.VMEM((PLANE, MINE, ROWS), bf16),
            pltpu.VMEM((PLANE, MINE, ROWS), bf16),
            pltpu.VMEM((PLANE, MINE, ROWS), bf16),
            pltpu.VMEM((C, X, Z, Y, 16, 256), bf16),
            pltpu.VMEM((X * C, 16, 128), bf16),
            pltpu.VMEM((RANK, 2 * MINE), bf16),
            pltpu.VMEM((2 * MINE, 128), f32),
            pltpu.VMEM((MINE, 128), f32),
            pltpu.VMEM((D_MODEL // 128, 128), f32),
            pltpu.VMEM((RANK, ROWS), bf16),
            pltpu.VMEM((1, PIECE), f32),
            pltpu.VMEM((1, PIECE), f32),
            dma((STEPS,)), dma((4,)), dma((PLANE,)), dma((PLANE,)), dma((PLANE,)), dma((PLANE,)),
            dma((X * C,)), dma((X * C,)), dma((hops,)), dma((hops,)),
        ],
        compiler_params=pltpu.CompilerParams(
            collective_id=0, has_side_effects=True, vmem_limit_bytes=40 * 2**20
        ),
        name="exchange",
    )(*(pltpu.with_memory_space_constraint(a, pltpu.HBM) for a in operands))
    serve_t, scale, norm = pl.pallas_call(
        scale_kernel,
        grid=(WRITES,),
        out_shape=(
            jax.ShapeDtypeStruct((MINE, D_MODEL), bf16),
            jax.ShapeDtypeStruct((1, MINE), f32),
            jax.ShapeDtypeStruct((D_MODEL // 128, 128), bf16),
        ),
        in_specs=[vmem] * 4,
        out_specs=(
            pl.BlockSpec((MINE, D_MODEL // WRITES), lambda i: (0, i)),
            pl.BlockSpec((1, MINE), lambda i: (0, 0)),
            pl.BlockSpec((D_MODEL // 128, 128), lambda i: (0, 0)),
        ),
        compiler_params=pltpu.CompilerParams(vmem_limit_bytes=12 * 2**20),
        name="rescale",
    )(*found)
    return serve_t.T, scale.reshape(-1), norm.reshape(-1)


def solution(mesh):
    split = Mesh(mesh.devices.reshape(Z, Y, X, C), ("z", "y", "x", "c"))
    rows, cols = ("z", "y"), ("x", "c")
    in_specs = (P(rows, cols), P(rows, None), P(None, cols), P(rows + cols), P(rows + cols))
    out_specs = (P(None, cols + rows), P(cols + rows), P())
    return jax.shard_map(per_device, mesh=split, in_specs=in_specs, out_specs=out_specs, check_vma=False)
```

```python
import functools

import jax
import jax.numpy as jnp
from jax import lax
from jax.experimental import pallas as pl
from jax.experimental.pallas import tpu as pltpu
from jax.sharding import Mesh
from jax.sharding import PartitionSpec as P

MESH = pl.DeviceIdType.MESH
Z, Y, X, C = 8, 4, 4, 2
PLANE = Z * Y
D_MODEL, RANK = 12288, 64
ROWS = D_MODEL // PLANE
COLS = 6144
MINE = COLS // PLANE
PIECE = D_MODEL // (PLANE * X * C)
STEPS = PLANE // 2
AWAY = (5, 1, 6, 2, 7, 3, 4, 0)
NEAR_FIRST = (7, 1, 6, 2, 5, 3, 4, 0)
WRITES = 2

mix_rate = 0.5


def comm_kernel(
    w_hbm, low_hbm, high_hbm, train_hbm, step_hbm,
    fresh_ref, inv_ref, scale_ref, norm_ref,
    wbuf, stage, recv, relay, lowbuf, nbuf, hpair, ht, acc, norms, low_ref, nt_ref, ns_ref,
    wsem, isem, zsend, zrecv, ysend, yrecv, nsend, nrecv, psend, precv,
):
    z, y = lax.axis_index("z"), lax.axis_index("y")
    x, c = lax.axis_index("x"), lax.axis_index("c")
    row = z * Y + y
    me = x * C + c

    def step(s):
        return away(s % Z if isinstance(s, int) else lax.rem(s, Z)), 1 - s // Z

    def step_of(dz, q):
        return listed(dz, [AWAY.index(k) for k in range(Z)]) + (1 - q) * Z

    def away(k):
        return listed(k, AWAY)

    def listed(k, table):
        if isinstance(k, int):
            return table[k]
        found = jnp.int32(table[0])
        for n in range(1, Z):
            found = jnp.where(k == n, table[n], found)
        return found

    def partner(dz, q, j):
        return lax.rem(z + dz, Z), 2 * lax.rem(y // 2 + q, 2) + lax.rem(y + j, 2)

    def side_device(k):
        other = lax.rem(me + k, X * C)
        return {"x": other // C, "c": lax.rem(other, C)}

    def pair_of(s):
        dz, q = step(s)
        to_z, to_y = partner(dz, q, 0)
        return to_z * (Y // 2) + to_y // 2

    def weight_copy(s):
        return pltpu.make_async_copy(
            w_hbm.at[:, pl.ds(pl.multiple_of(pair_of(s) * 2 * MINE, 128), 2 * MINE)], wbuf.at[s], wsem.at[s]
        )

    for s in range(2):
        weight_copy(s).start()

    barrier = pltpu.get_barrier_semaphore()
    for k in range(1, Z):
        pl.semaphore_signal(barrier, inc=1, device_id={"z": lax.rem(z + k, Z)}, device_id_type=MESH)
    for k in range(1, Y):
        pl.semaphore_signal(barrier, inc=1, device_id={"y": lax.rem(y + k, Y)}, device_id_type=MESH)
    for k in range(1, X * C):
        pl.semaphore_signal(barrier, inc=1, device_id=side_device(k), device_id_type=MESH)

    pair = high_hbm.at[:, pl.ds(pl.multiple_of((row // 2) * 2 * MINE, 128), 2 * MINE)]
    small = [
        pltpu.make_async_copy(ref, to, isem.at[k])
        for k, (ref, to) in enumerate(((train_hbm, nt_ref), (step_hbm, ns_ref), (low_hbm, low_ref), (pair, hpair)))
    ]
    for copy in small:
        copy.start()
    for s in range(2, STEPS):
        weight_copy(s).start()

    def turn(s):
        weight_copy(s).wait()
        turned = wbuf[s].T
        stage[2 * s] = turned[0:MINE]
        stage[2 * s + 1] = turned[MINE : 2 * MINE]

    def copy_z(dz, e, into):
        q, j = e // 2, lax.rem(e, 2)
        to_z, to_y = partner(dz, q, j)
        slot = dz * Y + e
        return pltpu.make_async_remote_copy(
            src_ref=stage.at[2 * step_of(dz, q) + lax.rem(to_y, 2)], dst_ref=into.at[slot],
            send_sem=zsend.at[slot], recv_sem=zrecv.at[slot], device_id={"z": to_z}, device_id_type=MESH,
        )

    def copy_y(ref, dz, e):
        slot = dz * Y + e
        return pltpu.make_async_remote_copy(
            src_ref=ref, dst_ref=recv.at[slot], send_sem=ysend.at[slot], recv_sem=yrecv.at[slot],
            device_id={"y": partner(dz, e // 2, lax.rem(e, 2))[1]}, device_id_type=MESH,
        )

    def each(first, last, do):
        @pl.loop(first, last)
        def _(k):
            do(k)

    def turn_and_send(first, last, e):
        @pl.loop(first, last)
        def _(s):
            turn(s)
            copy_z(step(s - 1)[0], e, relay).start()

    turn(0)
    turn(1)
    pl.semaphore_wait(barrier, Z - 1 + Y - 1 + X * C - 1)
    copy_z(away(0), 2, relay).start()
    turn_and_send(2, 4, 2)

    for copy in small:
        copy.wait()
    gain = (nt_ref[...] + ns_ref[...]).astype(jnp.bfloat16).astype(jnp.float32)
    spot = me * PIECE + lax.broadcasted_iota(jnp.int32, (16, PIECE), 1)
    in_row = spot // 128 == lax.broadcasted_iota(jnp.int32, (16, PIECE), 0)
    left = jnp.where(in_row, jnp.broadcast_to(gain, (16, PIECE)), 0.0).astype(jnp.bfloat16)
    lane = lax.rem(me * PIECE + lax.broadcasted_iota(jnp.int32, (PIECE, 128), 0), 128)
    right = jnp.where(lane == lax.broadcasted_iota(jnp.int32, (PIECE, 128), 1), 1.0, 0.0).astype(jnp.bfloat16)
    nbuf[me] = jnp.dot(left, right, preferred_element_type=jnp.float32).astype(jnp.bfloat16)

    ranks = pl.ds(pl.multiple_of(x * 16, 16), 16)

    @pl.when(c == 0)
    def _():
        lowbuf[0, x, z, y] = low_ref[ranks, 0:256]

    @pl.when(c == 1)
    def _():
        lowbuf[1, x, z, y, :, 0:128] = low_ref[ranks, 256:384]

    def gain_copy(k):
        return pltpu.make_async_remote_copy(
            src_ref=nbuf.at[me], dst_ref=nbuf.at[me], send_sem=nsend.at[k], recv_sem=nrecv.at[k],
            device_id=side_device(k), device_id_type=MESH,
        )

    for k in range(1, X * C):
        gain_copy(k).start()
    turn_and_send(4, Z, 2)
    for k in range(1, X * C):
        gain_copy(k).wait()
    gains = nbuf[0].astype(jnp.float32)
    for k in range(1, X * C):
        gains = gains + nbuf[k].astype(jnp.float32)

    @pl.when(c == 1)
    def _():
        lowbuf[1, x, z, y, :, 128:256] = gains.astype(jnp.bfloat16)

    def hop_copy(ref, slot, device):
        return pltpu.make_async_remote_copy(
            src_ref=ref, dst_ref=ref, send_sem=psend.at[slot], recv_sem=precv.at[slot],
            device_id=device, device_id_type=MESH,
        )

    along_z = [hop_copy(lowbuf.at[c, x, z, y], k - 1, {"z": lax.rem(z + k, Z)}) for k in range(1, Z)]
    along_y = [hop_copy(lowbuf.at[c, x, :, y], Z - 2 + k, {"y": lax.rem(y + k, Y)}) for k in range(1, Y)]
    aside = [hop_copy(lowbuf.at[c, x], Z + Y - 3 + k, side_device(k)) for k in range(1, X * C)]
    for copy in along_z:
        copy.start()
    each(0, Z - 1, lambda k: copy_z(away(k), 3, relay).start())
    beside = [copy_y(stage.at[2 * step_of(0, e // 2) + lax.rem(y + e % 2, 2)], 0, e) for e in range(1, Y)]
    for copy in beside[1:]:
        copy.start()
    turn(Z)
    turn_and_send(Z + 1, STEPS, 1)
    def last_away(k):
        return jnp.where(lax.rem(z + 1, Z) <= Z // 2, listed(k, NEAR_FIRST), listed(Z - 2 - k, NEAR_FIRST))

    each(0, Z - 1, lambda k: copy_z(last_away(k), 0, recv).start())
    beside[0].start()

    wide = jnp.concatenate([hpair[...].astype(jnp.float32), jnp.zeros((RANK, 2 * MINE), jnp.float32)], axis=0)
    ht[...] = wide.T
    mine = pl.ds(pl.multiple_of(lax.rem(row, 2) * MINE, 8), MINE)
    high_t = ht[mine, :][:, 0:RANK].astype(jnp.bfloat16)

    for copy in along_z:
        copy.wait()
    for copy in along_y:
        copy.start()

    def pass_on(dz, e):
        copy_z(dz, e, relay).wait_recv()
        copy_y(relay.at[dz * Y + e], dz, e).start()

    each(0, Z - 1, lambda k: pass_on(away(k), 2))
    for copy in along_y:
        copy.wait()
    for copy in aside:
        copy.start()
    each(0, Z - 1, lambda k: pass_on(away(k), 3))
    for copy in aside:
        copy.wait()

    acc[...] = jnp.zeros_like(acc)

    def add_block(block, from_z, from_y):
        low = jnp.concatenate(
            [
                jnp.concatenate([lowbuf[0, k, from_z, from_y], lowbuf[1, k, from_z, from_y, :, 0:128]], axis=1)
                for k in range(X)
            ],
            axis=0,
        )
        fresh = block.astype(jnp.float32) + mix_rate * jnp.dot(high_t, low, preferred_element_type=jnp.float32)
        from_row = from_z * Y + from_y
        fresh_ref[:, pl.ds(pl.multiple_of(from_row * ROWS, 128), ROWS)] = fresh
        square = fresh * fresh
        acc[...] += square[:, 0:128] + square[:, 128:256] + square[:, 256:384]

    @pl.loop(0, PLANE)
    def _(r):
        norms[pl.ds(r * 3, 3), :] = lowbuf[1, 0, r // Y, lax.rem(r, Y), :, 128:256].astype(jnp.float32)[0:3]

    norm_ref[...] = norms[...].astype(jnp.bfloat16)

    def add_from(dz, e):
        add_block(recv[dz * Y + e], lax.rem(z + Z - dz, Z), partner(dz, e // 2, lax.rem(e, 2))[1])

    def add_passed(dz, e):
        copy_y(relay.at[dz * Y + e], dz, e).wait_recv()
        add_from(dz, e)

    def pass_and_add(k):
        dz = away(k)
        pass_on(dz, 1)
        add_passed(dz, 2)
        add_passed(dz, 3)

    def add_last(k):
        dz = away(k)
        copy_z(dz, 0, recv).wait_recv()
        add_from(dz, 0)

    add_block(stage[2 * step_of(0, 0) + lax.rem(y, 2)], z, y)
    each(1, Y, lambda e: add_passed(0, e))
    each(0, Z - 1, pass_and_add)
    each(0, Z - 1, lambda k: add_passed(away(k), 1))
    def sent(slot):
        @pl.when(lax.rem(slot, Y) > 0)
        def _():
            copy_y(relay.at[slot], slot // Y, lax.rem(slot, Y)).wait_send()

            @pl.when(slot > Y)
            def _():
                copy_z(slot // Y, lax.rem(slot, Y), recv).wait_send()

    each(0, PLANE, sent)
    each(0, Z - 1, add_last)

    for dz in range(1, Z):
        copy_z(dz, 0, recv).wait_send()

    scale = jnp.broadcast_to(jnp.sqrt(jnp.sum(acc[...], axis=1, keepdims=True)), (MINE, 128))
    inv_ref[...] = 1.0 / scale
    scale_ref[...] = jnp.concatenate([scale, jnp.zeros((64, 128), jnp.float32)], axis=0).T[0:8]


def scale_kernel(fresh_ref, inv_ref, scale_ref, norm_ref, serve_ref, scale_out, norm_out):
    width = serve_ref.shape[1]
    at = pl.program_id(0) * width
    inv = inv_ref[...]
    for k in range(width // 128):
        part = fresh_ref[:, pl.ds(pl.multiple_of(at + k * 128, 128), 128)]
        serve_ref[:, k * 128 : (k + 1) * 128] = (part * inv).astype(jnp.bfloat16)

    @pl.when(pl.program_id(0) == 0)
    def _():
        scale_out[...] = scale_ref[0:1, 0:MINE]
        norm_out[...] = norm_ref[...]


def per_device(weight_up, low_up, high_up, norm_train, norm_step):
    vmem = pl.BlockSpec(memory_space=pltpu.VMEM)
    hbm = pl.BlockSpec(memory_space=pltpu.HBM)
    bf16, f32 = jnp.bfloat16, jnp.float32
    dma = pltpu.SemaphoreType.DMA
    operands = weight_up, low_up.T, high_up, norm_train.reshape(1, PIECE), norm_step.reshape(1, PIECE)
    hops = Z + Y + X * C - 3
    found = pl.pallas_call(
        comm_kernel,
        out_shape=(
            pltpu.VMEM((MINE, D_MODEL), f32),
            pltpu.VMEM((MINE, 128), f32),
            pltpu.VMEM((8, 256), f32),
            pltpu.VMEM((D_MODEL // 128, 128), bf16),
        ),
        in_specs=[hbm] * 5,
        out_specs=(vmem, vmem, vmem, vmem),
        scratch_shapes=[
            pltpu.VMEM((STEPS, ROWS, 2 * MINE), bf16),
            pltpu.VMEM((PLANE, MINE, ROWS), bf16),
            pltpu.VMEM((PLANE, MINE, ROWS), bf16),
            pltpu.VMEM((PLANE, MINE, ROWS), bf16),
            pltpu.VMEM((C, X, Z, Y, 16, 256), bf16),
            pltpu.VMEM((X * C, 16, 128), bf16),
            pltpu.VMEM((RANK, 2 * MINE), bf16),
            pltpu.VMEM((2 * MINE, 128), f32),
            pltpu.VMEM((MINE, 128), f32),
            pltpu.VMEM((D_MODEL // 128, 128), f32),
            pltpu.VMEM((RANK, ROWS), bf16),
            pltpu.VMEM((1, PIECE), f32),
            pltpu.VMEM((1, PIECE), f32),
            dma((STEPS,)), dma((4,)), dma((PLANE,)), dma((PLANE,)), dma((PLANE,)), dma((PLANE,)),
            dma((X * C,)), dma((X * C,)), dma((hops,)), dma((hops,)),
        ],
        compiler_params=pltpu.CompilerParams(
            collective_id=0, has_side_effects=True, vmem_limit_bytes=40 * 2**20
        ),
        name="exchange",
    )(*(pltpu.with_memory_space_constraint(a, pltpu.HBM) for a in operands))
    serve_t, scale, norm = pl.pallas_call(
        scale_kernel,
        grid=(WRITES,),
        out_shape=(
            jax.ShapeDtypeStruct((MINE, D_MODEL), bf16),
            jax.ShapeDtypeStruct((1, MINE), f32),
            jax.ShapeDtypeStruct((D_MODEL // 128, 128), bf16),
        ),
        in_specs=[vmem] * 4,
        out_specs=(
            pl.BlockSpec((MINE, D_MODEL // WRITES), lambda i: (0, i)),
            pl.BlockSpec((1, MINE), lambda i: (0, 0)),
            pl.BlockSpec((D_MODEL // 128, 128), lambda i: (0, 0)),
        ),
        compiler_params=pltpu.CompilerParams(vmem_limit_bytes=12 * 2**20),
        name="rescale",
    )(*found)
    return serve_t.T, scale.reshape(-1), norm.reshape(-1)


def solution(mesh):
    split = Mesh(mesh.devices.reshape(Z, Y, X, C), ("z", "y", "x", "c"))
    rows, cols = ("z", "y"), ("x", "c")
    in_specs = (P(rows, cols), P(rows, None), P(None, cols), P(rows + cols), P(rows + cols))
    out_specs = (P(None, cols + rows), P(cols + rows), P())
    return jax.shard_map(per_device, mesh=split, in_specs=in_specs, out_specs=out_specs, check_vma=False)
```
